32 devices in a mesh: tm: 8 (over z, y), node: 4 (over x, core).
Axes of the slice: x: 2, y: 2, z: 4, core: 2. Of those that a mesh axis runs over, the one named last changes fastest.
Arguments:
- slice_starts: float32 [8, 32, 16384], P('tm'), may hold values from -1 to 1
- coupling: float32 [32, 16384], replicated, may hold values from 0.03 to 0.25
Outputs:
- node_values: float32 [8, 4, 32, 16384], P('tm', 'node')
- residual_log: float32 [3, 32], replicated
The draws below stay inside these ranges and needn't reach their ends.
All inputs are finite; a program needn't handle non-finite values.
Results may differ from the reference program's by a relative error of at most 0.0001.
Values sent between devices are 32-bit elements.
A program may use at most 128 MiB of HBM per device.

```python
import math
import jax
import jax.numpy as jnp
from jax import lax

X = 16384
SYS = 32
M = 4
SWEEPS = 3
NEWTON = 2
SLICES = 8


def block_scale(stream_key, shape, pieces, least, top_value):
    level, own = 1.0, jax.random.fold_in(stream_key, 6)
    for position, shards_of in pieces:
        draws = jnp.exp(jax.random.uniform(jax.random.fold_in(own, position), (shards_of,), jnp.float32, least / len(pieces), top_value / len(pieces)))
        level = level * jnp.repeat(draws, shape[position] // shards_of).reshape([-1 if axis == position else 1 for axis in range(len(shape))])
    return level


def setup_inputs(seed: int = 0) -> dict:
    key_of = jax.random.split(jax.random.key(seed), 3)
    return {
        "slice_starts": jnp.clip(jax.random.uniform(key_of[0], (SLICES, SYS, X), jnp.float32, -1.0, 1.0) * block_scale(key_of[0], (SLICES, SYS, X), ((0, 8),), -0.4, 0.0), -1.0, 1.0),
        "coupling": jnp.clip(jnp.exp(jax.random.uniform(key_of[1], (SYS, X), jnp.float32, math.log(0.03), math.log(0.25))), 0.03, 0.25),
    }


time_step = 0.5
log_floor = 0.05


def legendre_gap(point, node_count):
    before = 1.0
    current = point
    for degree in range(1, node_count):
        following = ((2 * degree + 1) * point * current - degree * before) / (degree + 1)
        before = current
        current = following
    return current - before


def collocation(node_count):
    points = []
    samples = 4000
    for sample_index in range(samples - 1):
        lower_end = -1.0 + 2.0 * sample_index / samples
        upper_end = -1.0 + 2.0 * (sample_index + 1) / samples
        lower_value = legendre_gap(lower_end, node_count)
        upper_value = legendre_gap(upper_end, node_count)
        if lower_value * upper_value < 0.0:
            for halving in range(80):
                middle = 0.5 * (lower_end + upper_end)
                middle_value = legendre_gap(middle, node_count)
                if lower_value * middle_value <= 0.0:
                    upper_end = middle
                else:
                    lower_end = middle
                    lower_value = middle_value
            points.append(0.5 * (lower_end + upper_end))
    points.append(1.0)
    node_times = [(point + 1.0) / 2.0 for point in points]
    matrix = [[0.0] * node_count for row_index in range(node_count)]
    for column in range(node_count):
        coeffs = [1.0]
        for other in range(node_count):
            if other != column:
                scale = node_times[column] - node_times[other]
                shifted = [0.0] + coeffs
                scaled = [value * node_times[other] for value in coeffs] + [0.0]
                coeffs = [(shifted[power] - scaled[power]) / scale for power in range(len(shifted))]
        for row_index in range(node_count):
            upper_time = node_times[row_index]
            matrix[row_index][column] = sum(coeffs[power] * upper_time ** (power + 1) / (power + 1) for power in range(len(coeffs)))
    return node_times, matrix


def operator_term(field_values, coupling):
    right_side = jnp.roll(field_values, -1, axis=-1)
    left_side = jnp.roll(field_values, 1, axis=-1)
    left_coupling = jnp.roll(coupling, 1, axis=-1)
    cubic = field_values * field_values * field_values
    return coupling * (right_side - field_values) - left_coupling * (field_values - left_side) + field_values - cubic


def reference(slice_starts, coupling):
    node_times, matrix = collocation(M)
    weights = jnp.asarray(matrix, jnp.float32)
    diag_weights = jnp.asarray([time_step * moment / M for moment in node_times], jnp.float32)
    implicit = diag_weights[None, :, None, None]
    node_state = jnp.broadcast_to(slice_starts[:, None], (SLICES, M, SYS, X))
    end_values = slice_starts
    residual_list = []
    for sweep_index in range(SWEEPS):
        starts = jnp.concatenate([slice_starts[:1], end_values[:-1]], axis=0)
        forcing = operator_term(node_state, coupling)
        quadrature = jnp.einsum("mj,pjsx->pmsx", weights, forcing, precision=lax.Precision.HIGHEST)
        base = starts[:, None] + time_step * quadrature
        defect = base - node_state
        mean_square = jnp.sum(defect * defect, axis=(0, 1, 3)) / (SLICES * M * X)
        residual_list.append(jnp.log(log_floor + mean_square))
        target = base - implicit * (node_state - node_state * node_state * node_state)
        iterate = node_state
        for newton_step in range(NEWTON):
            cubic = iterate * iterate * iterate
            derivative = 1.0 - implicit + 3.0 * implicit * iterate * iterate
            iterate = iterate - (iterate - implicit * (iterate - cubic) - target) / derivative
        node_state = iterate
        end_values = node_state[:, M - 1]
    return node_state, jnp.stack(residual_list)
```

```python
import functools
import jax
import jax.numpy as jnp
from jax import lax
from jax.experimental import pallas as pl
from jax.experimental.pallas import tpu as pltpu
from jax.sharding import PartitionSpec as P

M = 4
CHUNKS = 4
STEP = 4
LANE = 128
MESH = pl.DeviceIdType.MESH

time_step = 0.5
log_floor = 0.05


def legendre_gap(point, node_count):
    before = 1.0
    current = point
    for degree in range(1, node_count):
        following = ((2 * degree + 1) * point * current - degree * before) / (degree + 1)
        before = current
        current = following
    return current - before


def collocation(node_count):
    points = []
    samples = 4000
    for sample_index in range(samples - 1):
        lower_end = -1.0 + 2.0 * sample_index / samples
        upper_end = -1.0 + 2.0 * (sample_index + 1) / samples
        lower_value = legendre_gap(lower_end, node_count)
        upper_value = legendre_gap(upper_end, node_count)
        if lower_value * upper_value < 0.0:
            for halving in range(80):
                middle = 0.5 * (lower_end + upper_end)
                middle_value = legendre_gap(middle, node_count)
                if lower_value * middle_value <= 0.0:
                    upper_end = middle
                else:
                    lower_end = middle
                    lower_value = middle_value
            points.append(0.5 * (lower_end + upper_end))
    points.append(1.0)
    node_times = [(point + 1.0) / 2.0 for point in points]
    matrix = [[0.0] * node_count for row_index in range(node_count)]
    for column in range(node_count):
        coeffs = [1.0]
        for other in range(node_count):
            if other != column:
                scale = node_times[column] - node_times[other]
                shifted = [0.0] + coeffs
                scaled = [value * node_times[other] for value in coeffs] + [0.0]
                coeffs = [(shifted[power] - scaled[power]) / scale for power in range(len(shifted))]
        for row_index in range(node_count):
            upper_time = node_times[row_index]
            matrix[row_index][column] = sum(
                (
                    coeffs[power] * upper_time ** (power + 1) / (power + 1)
                    for power in range(len(coeffs))
                )
            )
    return (node_times, matrix)


def kernel(
    slices, rows, cells,
    start_hbm, coupling_hbm, out_hbm, log_ref,
    own, couple, prev1, prev2, prev3, here, there, mid, before, result,
    acc, part_tm, part_node,
    load_sem, s_prev1, r_prev1, s_prev2, r_prev2, s_prev3, r_prev3,
    s_out, r_out, local_sem, s_tm, r_tm, s_node, r_node,
):
    p = lax.axis_index("tm")
    n = lax.axis_index("node")
    chunk = cells // CHUNKS
    tiles = chunk // LANE
    span = chunk + 2 * LANE
    my_rows = pl.ds(pl.multiple_of(n * rows, rows), rows)
    node_times, matrix = collocation(M)
    weight = [[time_step * value for value in line] for line in matrix]
    total = [sum(line) for line in weight]
    implicit = [time_step * moment / M for moment in node_times]
    even = lax.rem(p, 2) == 0
    first = p == 0
    second = p == 1

    loads = []
    for index, (source, target) in enumerate(
        ((start_hbm.at[0, my_rows], own), (coupling_hbm.at[my_rows], couple))
    ):
        for piece, (lo, to, size) in enumerate(
            ((0, 2 * LANE, cells), (cells - LANE, LANE, LANE), (0, 2 * LANE + cells, LANE))
        ):
            copy = pltpu.make_async_copy(
                source.at[:, pl.ds(lo, size)],
                target.at[:, pl.ds(to, size)],
                load_sem.at[index, piece],
            )
            copy.start()
            loads.append(copy)

    barrier = pltpu.get_barrier_semaphore()
    for step in range(1, slices):
        pl.semaphore_signal(
            barrier, inc=1, device_id={"tm": lax.rem(p + step, slices), "node": n}, device_id_type=MESH
        )
    for step in range(1, M):
        pl.semaphore_signal(
            barrier, inc=1, device_id={"tm": p, "node": lax.rem(n + step, M)}, device_id_type=MESH
        )
    pl.semaphore_wait(barrier, slices - 1 + M - 1)
    for copy in loads:
        copy.wait()

    def remote(source, target, send, recv, tm, node):
        return pltpu.make_async_remote_copy(
            src_ref=source, dst_ref=target, send_sem=send, recv_sem=recv,
            device_id={"tm": tm, "node": node}, device_id_type=MESH,
        )

    partner = jnp.where(even, p + 1, p - 1)
    ahead = lax.rem(p + 2, slices)
    inner = pl.ds(LANE, span)

    def own_part(c):
        return own.at[:, pl.ds(c * chunk + LANE, span)]

    def to_partner_own(c):
        return remote(own_part(c), prev1.at[c, :, inner], s_prev1.at[c], r_prev1.at[c], partner, n)

    def to_partner_forward(c):
        return remote(prev2.at[c, :, inner], prev1.at[c, :, inner], s_prev1.at[c], r_prev1.at[c], partner, n)

    def ahead_own(c):
        return remote(own_part(c), prev2.at[c, :, inner], s_prev2.at[c], r_prev2.at[c], ahead, n)

    def ahead_forward(c):
        return remote(prev1.at[c, :, inner], prev3.at[c, :, inner], s_prev3.at[c], r_prev3.at[c], ahead, n)

    has_behind = p >= 2
    has_ahead = p + 2 < slices
    odd = jnp.logical_not(even)

    def start_ahead(c):
        @pl.when(has_ahead)
        def _():
            ahead_own(c).start()

    @pl.when(even)
    def _():
        for c in range(CHUNKS):
            to_partner_own(c).start()
    start_ahead(0)
    start_ahead(1)

    acc[...] = jnp.zeros_like(acc)

    def diffusion(v, c, k):
        size = (k + 2) * LANE
        right = pltpu.roll(v, size - 1, 1)
        flux = c * (right - v)
        left = pltpu.roll(flux, 1, 1)
        return (flux - left)[:, LANE:LANE + k * LANE]

    def two_steps(base, u, square, reaction, a):
        s = (3.0 * a) * square - a
        d = 1.0 + s
        top = base + u * s
        target = base - a * reaction
        dd = d * d
        tt = top * top
        above = target * (d * dd) + (2.0 * a) * (top * tt)
        below = d * ((1.0 - a) * dd + (3.0 * a) * tt)
        return above / below

    def folded(value, k):
        out = value[:, :LANE]
        for piece in range(1, k):
            out = out + value[:, piece * LANE:(piece + 1) * LANE]
        return out

    def over(count_tiles, block, edges):
        if edges:
            block(0, 1, False)
        def step(i, carry):
            block(1 + i * STEP, STEP, True)
            return carry
        lax.fori_loop(0, count_tiles // STEP, step, 0)
        if edges:
            block(count_tiles + 1, 1, False)

    def wide(tile, k):
        return pl.ds(pl.multiple_of(tile * LANE, LANE), (k + 2) * LANE)

    def centre(tile, k):
        return pl.ds(pl.multiple_of((tile + 1) * LANE, LANE), k * LANE)

    for c in range(CHUNKS):
        base_lane = c * chunk

        @pl.when(has_behind)
        def _():
            ahead_own(c).wait_recv()

        @pl.when(jnp.logical_and(odd, has_behind))
        def _():
            to_partner_forward(c).start()

        @pl.when(odd)
        def _():
            to_partner_own(c).wait_recv()

        @pl.when(jnp.logical_and(even, has_behind))
        def _():
            to_partner_forward(c).wait_recv()

        @pl.when(jnp.logical_and(has_ahead, jnp.logical_not(first)))
        def _():
            ahead_forward(c).start()
        if c + 2 < CHUNKS:
            start_ahead(c + 2)

        @pl.when(p >= 3)
        def _():
            ahead_forward(c).wait_recv()

        def own_wide(ref, tile, k):
            return ref[:, pl.ds(pl.multiple_of(base_lane + tile * LANE, LANE), (k + 2) * LANE)]

        def own_centre(ref, tile, k):
            return ref[:, pl.ds(pl.multiple_of(base_lane + (tile + 1) * LANE, LANE), k * LANE)]

        def stage_a(tile, k, counted):
            mid_slice = slice(LANE, LANE + k * LANE)
            cw = own_wide(couple, tile, k)
            at = centre(tile, k)
            vw = own_wide(own, tile, k)
            v = vw[:, mid_slice]
            p1w = jnp.where(first, vw, prev1[c, :, wide(tile, k)])
            p1 = p1w[:, mid_slice]
            p2w = jnp.where(p <= 1, p1w, prev2[c, :, wide(tile, k)])
            p2 = p2w[:, mid_slice]
            p3 = jnp.where(p <= 2, p2, prev3[c, :, at])

            square = v * v
            reaction = v - v * square
            forcing = diffusion(vw, cw, k) + reaction
            found = None
            for m in range(M):
                base = p1 + total[m] * forcing
                if counted:
                    defect = base - v
                    found = defect * defect if found is None else found + defect * defect
                here[m, :, at] = two_steps(base, v, square, reaction, implicit[m])
            if counted:
                acc[0] += folded(found, k)

            square = p1 * p1
            reaction = p1 - p1 * square
            forcing = diffusion(p1w, cw, k) + reaction
            for m in range(M):
                there[m, :, at] = two_steps(p2 + total[m] * forcing, p1, square, reaction, implicit[m])

            square = p2 * p2
            reaction = p2 - p2 * square
            forcing = diffusion(p2w, cw, k) + reaction
            last = two_steps(
                p3 + total[M - 1] * forcing, p2, square, reaction, implicit[M - 1]
            )
            before[:, at] = jnp.where(second, p1, last)

        over(tiles, stage_a, True)

        def update(source, begin, cw, tile, k, which, counted):
            values = []
            forcings = []
            for m in range(M):
                vw = source[m, :, wide(tile, k)]
                v = vw[:, LANE:LANE + k * LANE]
                square = v * v
                reaction = v - v * square
                values.append((v, square, reaction))
                forcings.append(diffusion(vw, cw, k) + reaction)
            found = None
            outputs = []
            for m in range(M):
                base = begin
                for j in range(M):
                    base = base + weight[m][j] * forcings[j]
                v, square, reaction = values[m]
                if counted:
                    defect = base - v
                    found = defect * defect if found is None else found + defect * defect
                outputs.append(two_steps(base, v, square, reaction, implicit[m]))
            if counted:
                acc[which] += folded(found, k)
            return outputs

        def stage_b(tile, k, counted):
            cw = own_wide(couple, tile, k)
            at = centre(tile, k)
            begin = jnp.where(first, own_centre(own, tile, k), there[M - 1, :, at])
            outputs = update(here, begin, cw, tile, k, 1, counted)
            for m in range(M):
                mid[m, :, at] = outputs[m]
            mixed = None
            mixed_reaction = None
            for m in range(M):
                w = weight[M - 1][m]
                vw = there[m, :, wide(tile, k)]
                v = vw[:, LANE:LANE + k * LANE]
                square = v * v
                reaction = v - v * square
                mixed = w * vw if mixed is None else mixed + w * vw
                mixed_reaction = w * reaction if mixed_reaction is None else mixed_reaction + w * reaction
            base = before[:, at] + (diffusion(mixed, cw, k) + mixed_reaction)
            last = two_steps(base, v, square, reaction, implicit[M - 1])
            before[:, at] = jnp.where(first, own_centre(own, tile, k), last)

        over(tiles, stage_b, True)

        def stage_c(tile, k, counted):
            cw = own_wide(couple, tile, k)
            outputs = update(mid, before[:, centre(tile, k)], cw, tile, k, 2, counted)
            at = pl.ds(pl.multiple_of((tile - 1) * LANE, LANE), k * LANE)
            for m in range(M):
                result[c, m, :, at] = outputs[m]

        over(tiles, stage_c, False)

        target = out_hbm.at[my_rows, pl.ds(base_lane, chunk)]
        for step in (2, 3, 1):
            peer = lax.rem(n + step, M)
            remote(result.at[c, peer], target, s_out.at[c, step], r_out.at[c, step], p, peer).start()
        pltpu.make_async_copy(result.at[c, n], target, local_sem.at[c]).start()

    lane = lax.broadcasted_iota(jnp.int32, (rows, LANE), 1)
    sub = lax.broadcasted_iota(jnp.int32, (rows, LANE), 0)
    place = lax.broadcasted_iota(jnp.int32, (8, LANE), 0)
    tile_value = jnp.zeros((8, LANE), jnp.float32)
    for which in range(3):
        per_system = jnp.sum(acc[which], axis=1, keepdims=True)
        row = jnp.sum(
            jnp.where(lane == n * rows + sub, per_system, 0.0), axis=0, keepdims=True
        )
        tile_value = tile_value + jnp.where(place == which, row, 0.0)
    part_tm[p] = tile_value
    sends = []
    for step in range(1, slices):
        copy = remote(
            part_tm.at[p], part_tm.at[p], s_tm.at[step], r_tm.at[step], lax.rem(p + step, slices), n
        )
        copy.start()
        sends.append(copy)
    for step in range(1, slices):
        source = lax.rem(p - step + slices, slices)
        remote(part_tm.at[source], part_tm.at[source], s_tm.at[step], r_tm.at[step], p, n).wait_recv()
    summed = part_tm[0]
    for index in range(1, slices):
        summed = summed + part_tm[index]
    part_node[n] = summed
    for step in range(1, M):
        copy = remote(
            part_node.at[n], part_node.at[n], s_node.at[step], r_node.at[step], p, lax.rem(n + step, M)
        )
        copy.start()
        sends.append(copy)
    for step in range(1, M):
        source = lax.rem(n - step + M, M)
        remote(part_node.at[source], part_node.at[source], s_node.at[step], r_node.at[step], p, n).wait_recv()
    summed = part_node[0]
    for index in range(1, M):
        summed = summed + part_node[index]
    log_ref[...] = jnp.log(log_floor + summed / (slices * M * cells))

    for copy in sends:
        copy.wait_send()
    for c in range(CHUNKS):
        here_rows = pl.ds(c * chunk, chunk)
        for step in range(1, M):
            source = lax.rem(n - step + M, M)
            landed = out_hbm.at[pl.ds(pl.multiple_of(source * rows, rows), rows), here_rows]
            arrived = remote(result.at[c, n], landed, s_out.at[c, step], r_out.at[c, step], p, n)
            arrived.wait_recv()
            arrived.wait_send()
        pltpu.make_async_copy(result.at[c, n], out_hbm.at[my_rows, here_rows], local_sem.at[c]).wait()

        @pl.when(has_ahead)
        def _():
            ahead_own(c).wait_send()

        @pl.when(jnp.logical_and(has_ahead, jnp.logical_not(first)))
        def _():
            ahead_forward(c).wait_send()

        @pl.when(even)
        def _():
            to_partner_own(c).wait_send()

        @pl.when(jnp.logical_and(odd, has_behind))
        def _():
            to_partner_forward(c).wait_send()


def solution(mesh):
    slices = mesh.shape["tm"]

    def body(slice_starts, coupling):
        systems, cells = coupling.shape
        rows = systems // M
        chunk = cells // CHUNKS
        padded = chunk + 4 * LANE
        f32 = jnp.float32
        dma = pltpu.SemaphoreType.DMA
        anywhere = pl.BlockSpec(memory_space=pl.ANY)
        values, logs = pl.pallas_call(
            functools.partial(kernel, slices, rows, cells),
            out_shape=(
                jax.ShapeDtypeStruct((systems, cells), f32),
                jax.ShapeDtypeStruct((8, LANE), f32),
            ),
            in_specs=[anywhere, anywhere],
            out_specs=(anywhere, pl.BlockSpec(memory_space=pltpu.VMEM)),
            scratch_shapes=[
                pltpu.VMEM((rows, cells + 4 * LANE), f32),
                pltpu.VMEM((rows, cells + 4 * LANE), f32),
                pltpu.VMEM((CHUNKS, rows, padded), f32),
                pltpu.VMEM((CHUNKS, rows, padded), f32),
                pltpu.VMEM((CHUNKS, rows, padded), f32),
                pltpu.VMEM((M, rows, padded), f32),
                pltpu.VMEM((M, rows, padded), f32),
                pltpu.VMEM((M, rows, padded), f32),
                pltpu.VMEM((rows, padded), f32),
                pltpu.VMEM((CHUNKS, M, rows, chunk), f32),
                pltpu.VMEM((3, rows, LANE), f32),
                pltpu.VMEM((slices, 8, LANE), f32),
                pltpu.VMEM((M, 8, LANE), f32),
                dma((2, 3)),
                dma((CHUNKS,)), dma((CHUNKS,)), dma((CHUNKS,)),
                dma((CHUNKS,)), dma((CHUNKS,)), dma((CHUNKS,)),
                dma((CHUNKS, M)), dma((CHUNKS, M)), dma((CHUNKS,)),
                dma((slices,)), dma((slices,)), dma((M,)), dma((M,)),
            ],
            compiler_params=pltpu.CompilerParams(
                collective_id=0, has_side_effects=True, vmem_limit_bytes=48 * 1024 * 1024
            ),
        )(slice_starts, coupling)
        return values[None, None], logs[:3, :systems]

    return jax.shard_map(
        body,
        mesh=mesh,
        in_specs=(P("tm", None, None), P()),
        out_specs=(P("tm", "node", None, None), P()),
        check_vma=False,
    )
```

```python
import functools
import jax
import jax.numpy as jnp
from jax import lax
from jax.experimental import pallas as pl
from jax.experimental.pallas import tpu as pltpu
from jax.sharding import PartitionSpec as P

M = 4
CHUNKS = 8
STEP = 4
LANE = 128
HALO = 3
PAD = 4
MESH = pl.DeviceIdType.MESH

time_step = 0.5
log_floor = 0.05


def legendre_gap(point, node_count):
    before = 1.0
    current = point
    for degree in range(1, node_count):
        following = ((2 * degree + 1) * point * current - degree * before) / (degree + 1)
        before = current
        current = following
    return current - before


def collocation(node_count):
    points = []
    samples = 4000
    for sample_index in range(samples - 1):
        lower_end = -1.0 + 2.0 * sample_index / samples
        upper_end = -1.0 + 2.0 * (sample_index + 1) / samples
        lower_value = legendre_gap(lower_end, node_count)
        upper_value = legendre_gap(upper_end, node_count)
        if lower_value * upper_value < 0.0:
            for halving in range(80):
                middle = 0.5 * (lower_end + upper_end)
                middle_value = legendre_gap(middle, node_count)
                if lower_value * middle_value <= 0.0:
                    upper_end = middle
                else:
                    lower_end = middle
                    lower_value = middle_value
            points.append(0.5 * (lower_end + upper_end))
    points.append(1.0)
    node_times = [(point + 1.0) / 2.0 for point in points]
    matrix = [[0.0] * node_count for row_index in range(node_count)]
    for column in range(node_count):
        coeffs = [1.0]
        for other in range(node_count):
            if other != column:
                scale = node_times[column] - node_times[other]
                shifted = [0.0] + coeffs
                scaled = [value * node_times[other] for value in coeffs] + [0.0]
                coeffs = [(shifted[power] - scaled[power]) / scale for power in range(len(shifted))]
        for row_index in range(node_count):
            upper_time = node_times[row_index]
            matrix[row_index][column] = sum(
                (
                    coeffs[power] * upper_time ** (power + 1) / (power + 1)
                    for power in range(len(coeffs))
                )
            )
    return (node_times, matrix)


def kernel(
    slices, rows, cells,
    start_hbm, coupling_hbm, out_hbm, log_ref,
    own, couple, prev1, prev2, prev3, here, there, mid, before, result,
    acc, part_tm, part_node,
    load_sem, s_prev1, r_prev1, s_prev2, r_prev2, s_prev3, r_prev3,
    s_out, r_out, local_sem, s_tm, r_tm, s_node, r_node,
):
    p = lax.axis_index("tm")
    n = lax.axis_index("node")
    chunk = cells // CHUNKS
    tiles = chunk // LANE
    all_tiles = cells // LANE
    my_rows = pl.ds(pl.multiple_of(n * rows, rows), rows)
    node_times, matrix = collocation(M)
    weight = [[time_step * value for value in line] for line in matrix]
    total = [sum(line) for line in weight]
    implicit = [time_step * moment / M for moment in node_times]
    even = lax.rem(p, 2) == 0
    first = p == 0
    second = p == 1

    loads = []
    for index, (source, target) in enumerate(
        ((start_hbm.at[0, my_rows], own), (coupling_hbm.at[my_rows], couple))
    ):
        for piece, (lo, to, size) in enumerate(
            ((0, PAD * LANE, cells), (cells - HALO * LANE, LANE, HALO * LANE), (0, PAD * LANE + cells, HALO * LANE))
        ):
            copy = pltpu.make_async_copy(
                source.at[:, pl.ds(lo, size)],
                target.at[:, pl.ds(to, size)],
                load_sem.at[index, piece],
            )
            copy.start()
            loads.append(copy)

    barrier = pltpu.get_barrier_semaphore()
    for step in range(1, slices):
        pl.semaphore_signal(
            barrier, inc=1, device_id={"tm": lax.rem(p + step, slices), "node": n}, device_id_type=MESH
        )
    for step in range(1, M):
        pl.semaphore_signal(
            barrier, inc=1, device_id={"tm": p, "node": lax.rem(n + step, M)}, device_id_type=MESH
        )
    pl.semaphore_wait(barrier, slices - 1 + M - 1)
    for copy in loads:
        copy.wait()

    def remote(source, target, send, recv, tm, node):
        return pltpu.make_async_remote_copy(
            src_ref=source, dst_ref=target, send_sem=send, recv_sem=recv,
            device_id={"tm": tm, "node": node}, device_id_type=MESH,
        )

    partner = jnp.where(even, p + 1, p - 1)
    ahead = lax.rem(p + 2, slices)

    def part(ref, c):
        begin = (c * tiles + HALO if c else -HALO) + PAD
        end = (c + 1) * tiles + HALO + PAD
        return ref.at[:, pl.ds(begin * LANE, (end - begin) * LANE)]

    def to_partner_own(c):
        return remote(part(own, c), part(prev1, c), s_prev1.at[c], r_prev1.at[c], partner, n)

    def to_partner_forward(c):
        return remote(part(prev2, c), part(prev1, c), s_prev1.at[c], r_prev1.at[c], partner, n)

    def ahead_own(c):
        return remote(part(own, c), part(prev2, c), s_prev2.at[c], r_prev2.at[c], ahead, n)

    def ahead_forward(c):
        return remote(part(prev1, c), part(prev3, c), s_prev3.at[c], r_prev3.at[c], ahead, n)

    has_behind = p >= 2
    has_ahead = p + 2 < slices
    odd = jnp.logical_not(even)

    def start_ahead(c):
        @pl.when(has_ahead)
        def _():
            ahead_own(c).start()

    @pl.when(even)
    def _():
        for c in range(CHUNKS):
            to_partner_own(c).start()
    def pass_across(c):
        @pl.when(has_behind)
        def _():
            ahead_own(c).wait_recv()

        @pl.when(jnp.logical_and(odd, has_behind))
        def _():
            to_partner_forward(c).start()

    def pass_ahead(c):
        @pl.when(odd)
        def _():
            to_partner_own(c).wait_recv()

        @pl.when(jnp.logical_and(even, has_behind))
        def _():
            to_partner_forward(c).wait_recv()

        @pl.when(jnp.logical_and(has_ahead, jnp.logical_not(first)))
        def _():
            ahead_forward(c).start()

    for c in range(3):
        start_ahead(c)

    acc[...] = jnp.zeros_like(acc)

    def diffusion(v, c, k):
        size = (k + 2) * LANE
        right = pltpu.roll(v, size - 1, 1)
        flux = c * (right - v)
        left = pltpu.roll(flux, 1, 1)
        return (flux - left)[:, LANE:LANE + k * LANE]

    def two_steps(base, u, square, reaction, a):
        s = (3.0 * a) * square - a
        d = 1.0 + s
        top = base + u * s
        target = base - a * reaction
        dd = d * d
        tt = top * top
        above = target * (d * dd) + (2.0 * a) * (top * tt)
        below = d * ((1.0 - a) * dd + (3.0 * a) * tt)
        guess = pl.reciprocal(below, approx=True)
        return above * (guess * (2.0 - below * guess))

    def folded(value, k):
        out = value[:, :LANE]
        for piece in range(1, k):
            out = out + value[:, piece * LANE:(piece + 1) * LANE]
        return out

    def run(begin, end, block, counted):
        count = (end - begin) // STEP

        def step(i, carry):
            block(begin + i * STEP, STEP, counted)
            return carry

        lax.fori_loop(0, count, step, 0)
        if begin + count * STEP < end:
            block(begin + count * STEP, end - begin - count * STEP, counted)

    def over(c, lag, block):
        begin = c * tiles + lag if c else 0
        end = min((c + 1) * tiles + lag, all_tiles)
        if c == 0 and lag:
            block(-lag, lag, False)
        run(begin, end, block, True)
        if c == CHUNKS - 1 and lag:
            block(all_tiles, lag, False)

    def lanes(offset):
        return offset * LANE if isinstance(offset, int) else pl.multiple_of(offset * LANE, LANE)

    def wide(tile, k):
        return pl.ds(lanes(tile + PAD - 1), (k + 2) * LANE)

    def centre(tile, k):
        return pl.ds(lanes(tile + PAD), k * LANE)

    pass_across(0)
    pass_across(1)
    pass_ahead(0)
    for c in range(CHUNKS):
        base_lane = c * chunk

        if c + 3 < CHUNKS:
            start_ahead(c + 3)
        if c + 2 < CHUNKS:
            pass_across(c + 2)
        if c + 1 < CHUNKS:
            pass_ahead(c + 1)

        @pl.when(p >= 3)
        def _():
            ahead_forward(c).wait_recv()

        def stage_a(tile, k, counted):
            mid_slice = slice(LANE, LANE + k * LANE)
            cw = couple[:, wide(tile, k)]
            at = centre(tile, k)
            vw = own[:, wide(tile, k)]
            v = vw[:, mid_slice]
            p1w = jnp.where(first, vw, prev1[:, wide(tile, k)])
            p1 = p1w[:, mid_slice]
            p2w = jnp.where(p <= 1, p1w, prev2[:, wide(tile, k)])
            p2 = p2w[:, mid_slice]
            p3 = jnp.where(p <= 2, p2, prev3[:, at])

            square = v * v
            reaction = v - v * square
            forcing = diffusion(vw, cw, k) + reaction
            found = None
            for m in range(M):
                base = p1 + total[m] * forcing
                if counted:
                    defect = base - v
                    found = defect * defect if found is None else found + defect * defect
                here[m, :, at] = two_steps(base, v, square, reaction, implicit[m])
            if counted:
                acc[0] += folded(found, k)

            square = p1 * p1
            reaction = p1 - p1 * square
            forcing = diffusion(p1w, cw, k) + reaction
            for m in range(M):
                there[m, :, at] = two_steps(p2 + total[m] * forcing, p1, square, reaction, implicit[m])

            square = p2 * p2
            reaction = p2 - p2 * square
            forcing = diffusion(p2w, cw, k) + reaction
            last = two_steps(
                p3 + total[M - 1] * forcing, p2, square, reaction, implicit[M - 1]
            )
            before[:, at] = jnp.where(second, p1, last)

        over(c, 2, stage_a)

        def update(source, begin, cw, tile, k, which, counted):
            values = []
            forcings = []
            for m in range(M):
                vw = source[m, :, wide(tile, k)]
                v = vw[:, LANE:LANE + k * LANE]
                square = v * v
                reaction = v - v * square
                values.append((v, square, reaction))
                forcings.append(diffusion(vw, cw, k) + reaction)
            found = None
            outputs = []
            for m in range(M):
                base = begin
                for j in range(M):
                    base = base + weight[m][j] * forcings[j]
                v, square, reaction = values[m]
                if counted:
                    defect = base - v
                    found = defect * defect if found is None else found + defect * defect
                outputs.append(two_steps(base, v, square, reaction, implicit[m]))
            if counted:
                acc[which] += folded(found, k)
            return outputs

        def stage_b(tile, k, counted):
            cw = couple[:, wide(tile, k)]
            at = centre(tile, k)
            begin = jnp.where(first, own[:, centre(tile, k)], there[M - 1, :, at])
            outputs = update(here, begin, cw, tile, k, 1, counted)
            for m in range(M):
                mid[m, :, at] = outputs[m]
            mixed = None
            mixed_reaction = None
            for m in range(M):
                w = weight[M - 1][m]
                vw = there[m, :, wide(tile, k)]
                v = vw[:, LANE:LANE + k * LANE]
                square = v * v
                reaction = v - v * square
                mixed = w * vw if mixed is None else mixed + w * vw
                mixed_reaction = w * reaction if mixed_reaction is None else mixed_reaction + w * reaction
            base = before[:, at] + (diffusion(mixed, cw, k) + mixed_reaction)
            last = two_steps(base, v, square, reaction, implicit[M - 1])
            before[:, at] = jnp.where(first, own[:, centre(tile, k)], last)

        over(c, 1, stage_b)

        def stage_c(tile, k, counted):
            cw = couple[:, wide(tile, k)]
            outputs = update(mid, before[:, centre(tile, k)], cw, tile, k, 2, counted)
            at = pl.ds(lanes(tile - c * tiles), k * LANE)
            for m in range(M):
                result[c, m, :, at] = outputs[m]

        over(c, 0, stage_c)

        target = out_hbm.at[my_rows, pl.ds(base_lane, chunk)]
        for step in (2, 3, 1):
            peer = lax.rem(n + step, M)
            remote(result.at[c, peer], target, s_out.at[c, step], r_out.at[c, step], p, peer).start()
        pltpu.make_async_copy(result.at[c, n], target, local_sem.at[c]).start()

    lane = lax.broadcasted_iota(jnp.int32, (rows, LANE), 1)
    sub = lax.broadcasted_iota(jnp.int32, (rows, LANE), 0)
    place = lax.broadcasted_iota(jnp.int32, (8, LANE), 0)
    tile_value = jnp.zeros((8, LANE), jnp.float32)
    for which in range(3):
        per_system = jnp.sum(acc[which], axis=1, keepdims=True)
        row = jnp.sum(
            jnp.where(lane == n * rows + sub, per_system, 0.0), axis=0, keepdims=True
        )
        tile_value = tile_value + jnp.where(place == which, row, 0.0)
    part_tm[p] = tile_value
    sends = []
    for step in range(1, slices):
        copy = remote(
            part_tm.at[p], part_tm.at[p], s_tm.at[step], r_tm.at[step], lax.rem(p + step, slices), n
        )
        copy.start()
        sends.append(copy)
    for step in range(1, slices):
        source = lax.rem(p - step + slices, slices)
        remote(part_tm.at[source], part_tm.at[source], s_tm.at[step], r_tm.at[step], p, n).wait_recv()
    summed = part_tm[0]
    for index in range(1, slices):
        summed = summed + part_tm[index]
    part_node[n] = summed
    for step in range(1, M):
        copy = remote(
            part_node.at[n], part_node.at[n], s_node.at[step], r_node.at[step], p, lax.rem(n + step, M)
        )
        copy.start()
        sends.append(copy)
    for step in range(1, M):
        source = lax.rem(n - step + M, M)
        remote(part_node.at[source], part_node.at[source], s_node.at[step], r_node.at[step], p, n).wait_recv()
    summed = part_node[0]
    for index in range(1, M):
        summed = summed + part_node[index]
    log_ref[...] = jnp.log(log_floor + summed / (slices * M * cells))

    for copy in sends:
        copy.wait_send()
    for c in range(CHUNKS):
        here_rows = pl.ds(c * chunk, chunk)
        for step in range(1, M):
            source = lax.rem(n - step + M, M)
            landed = out_hbm.at[pl.ds(pl.multiple_of(source * rows, rows), rows), here_rows]
            arrived = remote(result.at[c, n], landed, s_out.at[c, step], r_out.at[c, step], p, n)
            arrived.wait_recv()
            arrived.wait_send()
        pltpu.make_async_copy(result.at[c, n], out_hbm.at[my_rows, here_rows], local_sem.at[c]).wait()

        @pl.when(has_ahead)
        def _():
            ahead_own(c).wait_send()

        @pl.when(jnp.logical_and(has_ahead, jnp.logical_not(first)))
        def _():
            ahead_forward(c).wait_send()

        @pl.when(even)
        def _():
            to_partner_own(c).wait_send()

        @pl.when(jnp.logical_and(odd, has_behind))
        def _():
            to_partner_forward(c).wait_send()


def solution(mesh):
    slices = mesh.shape["tm"]

    def body(slice_starts, coupling):
        systems, cells = coupling.shape
        rows = systems // M
        chunk = cells // CHUNKS
        padded = cells + 2 * PAD * LANE
        f32 = jnp.float32
        dma = pltpu.SemaphoreType.DMA
        anywhere = pl.BlockSpec(memory_space=pl.ANY)
        values, logs = pl.pallas_call(
            functools.partial(kernel, slices, rows, cells),
            out_shape=(
                jax.ShapeDtypeStruct((systems, cells), f32),
                jax.ShapeDtypeStruct((8, LANE), f32),
            ),
            in_specs=[anywhere, anywhere],
            out_specs=(anywhere, pl.BlockSpec(memory_space=pltpu.VMEM)),
            scratch_shapes=[
                pltpu.VMEM((rows, padded), f32),
                pltpu.VMEM((rows, padded), f32),
                pltpu.VMEM((rows, padded), f32),
                pltpu.VMEM((rows, padded), f32),
                pltpu.VMEM((rows, padded), f32),
                pltpu.VMEM((M, rows, padded), f32),
                pltpu.VMEM((M, rows, padded), f32),
                pltpu.VMEM((M, rows, padded), f32),
                pltpu.VMEM((rows, padded), f32),
                pltpu.VMEM((CHUNKS, M, rows, chunk), f32),
                pltpu.VMEM((3, rows, LANE), f32),
                pltpu.VMEM((slices, 8, LANE), f32),
                pltpu.VMEM((M, 8, LANE), f32),
                dma((2, 3)),
                dma((CHUNKS,)), dma((CHUNKS,)), dma((CHUNKS,)),
                dma((CHUNKS,)), dma((CHUNKS,)), dma((CHUNKS,)),
                dma((CHUNKS, M)), dma((CHUNKS, M)), dma((CHUNKS,)),
                dma((slices,)), dma((slices,)), dma((M,)), dma((M,)),
            ],
            compiler_params=pltpu.CompilerParams(
                collective_id=0, has_side_effects=True, vmem_limit_bytes=48 * 1024 * 1024
            ),
        )(slice_starts, coupling)
        return values[None, None], logs[:3, :systems]

    return jax.shard_map(
        body,
        mesh=mesh,
        in_specs=(P("tm", None, None), P()),
        out_specs=(P("tm", "node", None, None), P()),
        check_vma=False,
    )
```

```python
import functools
import jax
import jax.numpy as jnp
from jax import lax
from jax.experimental import pallas as pl
from jax.experimental.pallas import tpu as pltpu
from jax.sharding import PartitionSpec as P

M = 4
CHUNKS = 8
STEP = 8
LANE = 128
HALO = 3
PAD = 4
MESH = pl.DeviceIdType.MESH

time_step = 0.5
log_floor = 0.05


def legendre_gap(point, node_count):
    before = 1.0
    current = point
    for degree in range(1, node_count):
        following = ((2 * degree + 1) * point * current - degree * before) / (degree + 1)
        before = current
        current = following
    return current - before


def collocation(node_count):
    points = []
    samples = 4000
    for sample_index in range(samples - 1):
        lower_end = -1.0 + 2.0 * sample_index / samples
        upper_end = -1.0 + 2.0 * (sample_index + 1) / samples
        lower_value = legendre_gap(lower_end, node_count)
        upper_value = legendre_gap(upper_end, node_count)
        if lower_value * upper_value < 0.0:
            for halving in range(80):
                middle = 0.5 * (lower_end + upper_end)
                middle_value = legendre_gap(middle, node_count)
                if lower_value * middle_value <= 0.0:
                    upper_end = middle
                else:
                    lower_end = middle
                    lower_value = middle_value
            points.append(0.5 * (lower_end + upper_end))
    points.append(1.0)
    node_times = [(point + 1.0) / 2.0 for point in points]
    matrix = [[0.0] * node_count for row_index in range(node_count)]
    for column in range(node_count):
        coeffs = [1.0]
        for other in range(node_count):
            if other != column:
                scale = node_times[column] - node_times[other]
                shifted = [0.0] + coeffs
                scaled = [value * node_times[other] for value in coeffs] + [0.0]
                coeffs = [(shifted[power] - scaled[power]) / scale for power in range(len(shifted))]
        for row_index in range(node_count):
            upper_time = node_times[row_index]
            matrix[row_index][column] = sum(
                (
                    coeffs[power] * upper_time ** (power + 1) / (power + 1)
                    for power in range(len(coeffs))
                )
            )
    return (node_times, matrix)


def kernel(
    slices, rows, cells,
    start_hbm, coupling_hbm, out_hbm, log_ref,
    own, couple, prev1, prev2, prev3, here, there, mid, before, result,
    acc, part_tm, part_node,
    load_sem, s_prev1, r_prev1, s_prev2, r_prev2, s_prev3, r_prev3,
    s_out, r_out, local_sem, s_tm, r_tm, s_node, r_node,
):
    p = lax.axis_index("tm")
    n = lax.axis_index("node")
    chunk = cells // CHUNKS
    tiles = chunk // LANE
    all_tiles = cells // LANE
    my_rows = pl.ds(pl.multiple_of(n * rows, rows), rows)
    node_times, matrix = collocation(M)
    weight = [[time_step * value for value in line] for line in matrix]
    total = [sum(line) for line in weight]
    implicit = [time_step * moment / M for moment in node_times]
    even = lax.rem(p, 2) == 0
    first = p == 0
    second = p == 1

    loads = []
    for index, (source, target) in enumerate(
        ((start_hbm.at[0, my_rows], own), (coupling_hbm.at[my_rows], couple))
    ):
        for piece, (lo, to, size) in enumerate(
            ((0, PAD * LANE, cells), (cells - HALO * LANE, LANE, HALO * LANE), (0, PAD * LANE + cells, HALO * LANE))
        ):
            copy = pltpu.make_async_copy(
                source.at[:, pl.ds(lo, size)],
                target.at[:, pl.ds(to, size)],
                load_sem.at[index, piece],
            )
            copy.start()
            loads.append(copy)

    barrier = pltpu.get_barrier_semaphore()
    for step in range(1, slices):
        pl.semaphore_signal(
            barrier, inc=1, device_id={"tm": lax.rem(p + step, slices), "node": n}, device_id_type=MESH
        )
    for step in range(1, M):
        pl.semaphore_signal(
            barrier, inc=1, device_id={"tm": p, "node": lax.rem(n + step, M)}, device_id_type=MESH
        )
    pl.semaphore_wait(barrier, slices - 1 + M - 1)
    for copy in loads:
        copy.wait()

    def remote(source, target, send, recv, tm, node):
        return pltpu.make_async_remote_copy(
            src_ref=source, dst_ref=target, send_sem=send, recv_sem=recv,
            device_id={"tm": tm, "node": node}, device_id_type=MESH,
        )

    partner = jnp.where(even, p + 1, p - 1)
    ahead = lax.rem(p + 2, slices)

    def part(ref, c):
        begin = (c * tiles + HALO if c else -HALO) + PAD
        end = (c + 1) * tiles + HALO + PAD
        return ref.at[:, pl.ds(begin * LANE, (end - begin) * LANE)]

    def to_partner_own(c):
        return remote(part(own, c), part(prev1, c), s_prev1.at[c], r_prev1.at[c], partner, n)

    def to_partner_forward(c):
        return remote(part(prev2, c), part(prev1, c), s_prev1.at[c], r_prev1.at[c], partner, n)

    def ahead_own(c):
        return remote(part(own, c), part(prev2, c), s_prev2.at[c], r_prev2.at[c], ahead, n)

    def ahead_forward(c):
        return remote(part(prev1, c), part(prev3, c), s_prev3.at[c], r_prev3.at[c], ahead, n)

    has_behind = p >= 2
    has_ahead = p + 2 < slices
    odd = jnp.logical_not(even)

    def start_ahead(c):
        @pl.when(has_ahead)
        def _():
            ahead_own(c).start()

    @pl.when(even)
    def _():
        for c in range(CHUNKS):
            to_partner_own(c).start()
    def pass_across(c):
        @pl.when(has_behind)
        def _():
            ahead_own(c).wait_recv()

        @pl.when(jnp.logical_and(odd, has_behind))
        def _():
            to_partner_forward(c).start()

    def pass_ahead(c):
        @pl.when(odd)
        def _():
            to_partner_own(c).wait_recv()

        @pl.when(jnp.logical_and(even, has_behind))
        def _():
            to_partner_forward(c).wait_recv()

        @pl.when(jnp.logical_and(has_ahead, jnp.logical_not(first)))
        def _():
            ahead_forward(c).start()

    for c in range(3):
        start_ahead(c)

    acc[...] = jnp.zeros_like(acc)

    def diffusion(v, c, k):
        size = (k + 2) * LANE
        right = pltpu.roll(v, size - 1, 1)
        flux = c * (right - v)
        left = pltpu.roll(flux, 1, 1)
        return (flux - left)[:, LANE:LANE + k * LANE]

    def two_steps(base, u, square, reaction, a):
        s = (3.0 * a) * square - a
        d = 1.0 + s
        top = base + u * s
        target = base - a * reaction
        dd = d * d
        tt = top * top
        above = target * (d * dd) + (2.0 * a) * (top * tt)
        below = d * ((1.0 - a) * dd + (3.0 * a) * tt)
        guess = pl.reciprocal(below, approx=True)
        return above * (guess * (2.0 - below * guess))

    def folded(value, k):
        out = value[:, :LANE]
        for piece in range(1, k):
            out = out + value[:, piece * LANE:(piece + 1) * LANE]
        return out

    def run(begin, end, block, counted):
        count = (end - begin) // STEP

        def step(i, carry):
            block(begin + i * STEP, STEP, counted)
            return carry

        lax.fori_loop(0, count, step, 0)
        if begin + count * STEP < end:
            block(begin + count * STEP, end - begin - count * STEP, counted)

    def over(c, lag, block):
        begin = c * tiles + lag if c else 0
        end = min((c + 1) * tiles + lag, all_tiles)
        if c == 0 and lag:
            block(-lag, lag, False)
        run(begin, end, block, True)
        if c == CHUNKS - 1 and lag:
            block(all_tiles, lag, False)

    def lanes(offset):
        return offset * LANE if isinstance(offset, int) else pl.multiple_of(offset * LANE, LANE)

    def wide(tile, k):
        return pl.ds(lanes(tile + PAD - 1), (k + 2) * LANE)

    def centre(tile, k):
        return pl.ds(lanes(tile + PAD), k * LANE)

    pass_across(0)
    pass_across(1)
    pass_ahead(0)
    for c in range(CHUNKS):
        base_lane = c * chunk

        if c + 3 < CHUNKS:
            start_ahead(c + 3)
        if c + 2 < CHUNKS:
            pass_across(c + 2)
        if c + 1 < CHUNKS:
            pass_ahead(c + 1)

        @pl.when(p >= 3)
        def _():
            ahead_forward(c).wait_recv()

        def stage_a(tile, k, counted):
            mid_slice = slice(LANE, LANE + k * LANE)
            cw = couple[:, wide(tile, k)]
            at = centre(tile, k)
            vw = own[:, wide(tile, k)]
            v = vw[:, mid_slice]
            p1w = jnp.where(first, vw, prev1[:, wide(tile, k)])
            p1 = p1w[:, mid_slice]
            p2w = jnp.where(p <= 1, p1w, prev2[:, wide(tile, k)])
            p2 = p2w[:, mid_slice]
            p3 = jnp.where(p <= 2, p2, prev3[:, at])

            square = v * v
            reaction = v - v * square
            forcing = diffusion(vw, cw, k) + reaction
            found = None
            for m in range(M):
                base = p1 + total[m] * forcing
                if counted:
                    defect = base - v
                    found = defect * defect if found is None else found + defect * defect
                here[m, :, at] = two_steps(base, v, square, reaction, implicit[m])
            if counted:
                acc[0] += folded(found, k)

            square = p1 * p1
            reaction = p1 - p1 * square
            forcing = diffusion(p1w, cw, k) + reaction
            for m in range(M):
                there[m, :, at] = two_steps(p2 + total[m] * forcing, p1, square, reaction, implicit[m])

            square = p2 * p2
            reaction = p2 - p2 * square
            forcing = diffusion(p2w, cw, k) + reaction
            last = two_steps(
                p3 + total[M - 1] * forcing, p2, square, reaction, implicit[M - 1]
            )
            before[:, at] = jnp.where(second, p1, last)

        over(c, 2, stage_a)

        def update(source, begin, cw, tile, k, which, counted):
            values = []
            forcings = []
            for m in range(M):
                vw = source[m, :, wide(tile, k)]
                v = vw[:, LANE:LANE + k * LANE]
                square = v * v
                reaction = v - v * square
                values.append((v, square, reaction))
                forcings.append(diffusion(vw, cw, k) + reaction)
            found = None
            outputs = []
            for m in range(M):
                base = begin
                for j in range(M):
                    base = base + weight[m][j] * forcings[j]
                v, square, reaction = values[m]
                if counted:
                    defect = base - v
                    found = defect * defect if found is None else found + defect * defect
                outputs.append(two_steps(base, v, square, reaction, implicit[m]))
            if counted:
                acc[which] += folded(found, k)
            return outputs

        def stage_b(tile, k, counted):
            cw = couple[:, wide(tile, k)]
            at = centre(tile, k)
            begin = jnp.where(first, own[:, centre(tile, k)], there[M - 1, :, at])
            outputs = update(here, begin, cw, tile, k, 1, counted)
            for m in range(M):
                mid[m, :, at] = outputs[m]
            mixed = None
            mixed_reaction = None
            for m in range(M):
                w = weight[M - 1][m]
                vw = there[m, :, wide(tile, k)]
                v = vw[:, LANE:LANE + k * LANE]
                square = v * v
                reaction = v - v * square
                mixed = w * vw if mixed is None else mixed + w * vw
                mixed_reaction = w * reaction if mixed_reaction is None else mixed_reaction + w * reaction
            base = before[:, at] + (diffusion(mixed, cw, k) + mixed_reaction)
            last = two_steps(base, v, square, reaction, implicit[M - 1])
            before[:, at] = jnp.where(first, own[:, centre(tile, k)], last)

        over(c, 1, stage_b)

        def stage_c(tile, k, counted):
            cw = couple[:, wide(tile, k)]
            outputs = update(mid, before[:, centre(tile, k)], cw, tile, k, 2, counted)
            at = pl.ds(lanes(tile - c * tiles), k * LANE)
            for m in range(M):
                result[c, m, :, at] = outputs[m]

        over(c, 0, stage_c)

        target = out_hbm.at[my_rows, pl.ds(base_lane, chunk)]
        for step in (2, 3, 1):
            peer = lax.rem(n + step, M)
            remote(result.at[c, peer], target, s_out.at[c, step], r_out.at[c, step], p, peer).start()
        pltpu.make_async_copy(result.at[c, n], target, local_sem.at[c]).start()

    lane = lax.broadcasted_iota(jnp.int32, (rows, LANE), 1)
    sub = lax.broadcasted_iota(jnp.int32, (rows, LANE), 0)
    place = lax.broadcasted_iota(jnp.int32, (8, LANE), 0)
    tile_value = jnp.zeros((8, LANE), jnp.float32)
    for which in range(3):
        per_system = jnp.sum(acc[which], axis=1, keepdims=True)
        row = jnp.sum(
            jnp.where(lane == n * rows + sub, per_system, 0.0), axis=0, keepdims=True
        )
        tile_value = tile_value + jnp.where(place == which, row, 0.0)
    part_tm[p] = tile_value
    sends = []
    for step in range(1, slices):
        copy = remote(
            part_tm.at[p], part_tm.at[p], s_tm.at[step], r_tm.at[step], lax.rem(p + step, slices), n
        )
        copy.start()
        sends.append(copy)
    for step in range(1, slices):
        source = lax.rem(p - step + slices, slices)
        remote(part_tm.at[source], part_tm.at[source], s_tm.at[step], r_tm.at[step], p, n).wait_recv()
    summed = part_tm[0]
    for index in range(1, slices):
        summed = summed + part_tm[index]
    part_node[n] = summed
    for step in range(1, M):
        copy = remote(
            part_node.at[n], part_node.at[n], s_node.at[step], r_node.at[step], p, lax.rem(n + step, M)
        )
        copy.start()
        sends.append(copy)
    for step in range(1, M):
        source = lax.rem(n - step + M, M)
        remote(part_node.at[source], part_node.at[source], s_node.at[step], r_node.at[step], p, n).wait_recv()
    summed = part_node[0]
    for index in range(1, M):
        summed = summed + part_node[index]
    log_ref[...] = jnp.log(log_floor + summed / (slices * M * cells))

    for copy in sends:
        copy.wait_send()
    for c in range(CHUNKS):
        here_rows = pl.ds(c * chunk, chunk)
        for step in range(1, M):
            source = lax.rem(n - step + M, M)
            landed = out_hbm.at[pl.ds(pl.multiple_of(source * rows, rows), rows), here_rows]
            arrived = remote(result.at[c, n], landed, s_out.at[c, step], r_out.at[c, step], p, n)
            arrived.wait_recv()
            arrived.wait_send()
        pltpu.make_async_copy(result.at[c, n], out_hbm.at[my_rows, here_rows], local_sem.at[c]).wait()

        @pl.when(has_ahead)
        def _():
            ahead_own(c).wait_send()

        @pl.when(jnp.logical_and(has_ahead, jnp.logical_not(first)))
        def _():
            ahead_forward(c).wait_send()

        @pl.when(even)
        def _():
            to_partner_own(c).wait_send()

        @pl.when(jnp.logical_and(odd, has_behind))
        def _():
            to_partner_forward(c).wait_send()


def solution(mesh):
    slices = mesh.shape["tm"]

    def body(slice_starts, coupling):
        systems, cells = coupling.shape
        rows = systems // M
        chunk = cells // CHUNKS
        padded = cells + 2 * PAD * LANE
        f32 = jnp.float32
        dma = pltpu.SemaphoreType.DMA
        anywhere = pl.BlockSpec(memory_space=pl.ANY)
        values, logs = pl.pallas_call(
            functools.partial(kernel, slices, rows, cells),
            out_shape=(
                jax.ShapeDtypeStruct((systems, cells), f32),
                jax.ShapeDtypeStruct((8, LANE), f32),
            ),
            in_specs=[anywhere, anywhere],
            out_specs=(anywhere, pl.BlockSpec(memory_space=pltpu.VMEM)),
            scratch_shapes=[
                pltpu.VMEM((rows, padded), f32),
                pltpu.VMEM((rows, padded), f32),
                pltpu.VMEM((rows, padded), f32),
                pltpu.VMEM((rows, padded), f32),
                pltpu.VMEM((rows, padded), f32),
                pltpu.VMEM((M, rows, padded), f32),
                pltpu.VMEM((M, rows, padded), f32),
                pltpu.VMEM((M, rows, padded), f32),
                pltpu.VMEM((rows, padded), f32),
                pltpu.VMEM((CHUNKS, M, rows, chunk), f32),
                pltpu.VMEM((3, rows, LANE), f32),
                pltpu.VMEM((slices, 8, LANE), f32),
                pltpu.VMEM((M, 8, LANE), f32),
                dma((2, 3)),
                dma((CHUNKS,)), dma((CHUNKS,)), dma((CHUNKS,)),
                dma((CHUNKS,)), dma((CHUNKS,)), dma((CHUNKS,)),
                dma((CHUNKS, M)), dma((CHUNKS, M)), dma((CHUNKS,)),
                dma((slices,)), dma((slices,)), dma((M,)), dma((M,)),
            ],
            compiler_params=pltpu.CompilerParams(
                collective_id=0, has_side_effects=True, vmem_limit_bytes=48 * 1024 * 1024
            ),
        )(slice_starts, coupling)
        return values[None, None], logs[:3, :systems]

    return jax.shard_map(
        body,
        mesh=mesh,
        in_specs=(P("tm", None, None), P()),
        out_specs=(P("tm", "node", None, None), P()),
        check_vma=False,
    )
```

```python
import functools
import jax
import jax.numpy as jnp
from jax import lax
from jax.experimental import pallas as pl
from jax.experimental.pallas import tpu as pltpu
from jax.sharding import PartitionSpec as P

M = 4
CHUNKS = 8
STEP = 8
LANE = 128
HALO = 3
PAD = 4
MESH = pl.DeviceIdType.MESH

time_step = 0.5
log_floor = 0.05


def legendre_gap(point, node_count):
    before = 1.0
    current = point
    for degree in range(1, node_count):
        following = ((2 * degree + 1) * point * current - degree * before) / (degree + 1)
        before = current
        current = following
    return current - before


def collocation(node_count):
    points = []
    samples = 4000
    for sample_index in range(samples - 1):
        lower_end = -1.0 + 2.0 * sample_index / samples
        upper_end = -1.0 + 2.0 * (sample_index + 1) / samples
        lower_value = legendre_gap(lower_end, node_count)
        upper_value = legendre_gap(upper_end, node_count)
        if lower_value * upper_value < 0.0:
            for halving in range(80):
                middle = 0.5 * (lower_end + upper_end)
                middle_value = legendre_gap(middle, node_count)
                if lower_value * middle_value <= 0.0:
                    upper_end = middle
                else:
                    lower_end = middle
                    lower_value = middle_value
            points.append(0.5 * (lower_end + upper_end))
    points.append(1.0)
    node_times = [(point + 1.0) / 2.0 for point in points]
    matrix = [[0.0] * node_count for row_index in range(node_count)]
    for column in range(node_count):
        coeffs = [1.0]
        for other in range(node_count):
            if other != column:
                scale = node_times[column] - node_times[other]
                shifted = [0.0] + coeffs
                scaled = [value * node_times[other] for value in coeffs] + [0.0]
                coeffs = [(shifted[power] - scaled[power]) / scale for power in range(len(shifted))]
        for row_index in range(node_count):
            upper_time = node_times[row_index]
            matrix[row_index][column] = sum(
                (
                    coeffs[power] * upper_time ** (power + 1) / (power + 1)
                    for power in range(len(coeffs))
                )
            )
    return (node_times, matrix)


def kernel(
    slices, rows, cells,
    start_hbm, coupling_hbm, out_hbm, log_ref,
    own, couple, prev1, prev2, prev3, here, there, mid, before, result,
    acc, part_tm, part_node,
    load_sem, s_prev1, r_prev1, s_prev2, r_prev2, s_prev3, r_prev3,
    s_out, r_out, local_sem, s_tm, r_tm, s_node, r_node,
):
    p = lax.axis_index("tm")
    n = lax.axis_index("node")
    chunk = cells // CHUNKS
    tiles = chunk // LANE
    all_tiles = cells // LANE
    my_rows = pl.ds(pl.multiple_of(n * rows, rows), rows)
    node_times, matrix = collocation(M)
    weight = [[time_step * value for value in line] for line in matrix]
    total = [sum(line) for line in weight]
    implicit = [time_step * moment / M for moment in node_times]
    even = lax.rem(p, 2) == 0
    first = p == 0
    second = p == 1

    loads = []
    for index, (source, target) in enumerate(
        ((start_hbm.at[0, my_rows], own), (coupling_hbm.at[my_rows], couple))
    ):
        for piece, (lo, to, size) in enumerate(
            ((0, PAD * LANE, cells), (cells - HALO * LANE, LANE, HALO * LANE), (0, PAD * LANE + cells, HALO * LANE))
        ):
            copy = pltpu.make_async_copy(
                source.at[:, pl.ds(lo, size)],
                target.at[:, pl.ds(to, size)],
                load_sem.at[index, piece],
            )
            copy.start()
            loads.append(copy)

    barrier = pltpu.get_barrier_semaphore()
    for step in range(1, slices):
        pl.semaphore_signal(
            barrier, inc=1, device_id={"tm": lax.rem(p + step, slices), "node": n}, device_id_type=MESH
        )
    for step in range(1, M):
        pl.semaphore_signal(
            barrier, inc=1, device_id={"tm": p, "node": lax.rem(n + step, M)}, device_id_type=MESH
        )
    pl.semaphore_wait(barrier, slices - 1 + M - 1)
    for copy in loads:
        copy.wait()

    def remote(source, target, send, recv, tm, node):
        return pltpu.make_async_remote_copy(
            src_ref=source, dst_ref=target, send_sem=send, recv_sem=recv,
            device_id={"tm": tm, "node": node}, device_id_type=MESH,
        )

    partner = jnp.where(even, p + 1, p - 1)
    ahead = lax.rem(p + 2, slices)

    def part(ref, c):
        begin = (c * tiles + HALO if c else -HALO) + PAD
        end = (c + 1) * tiles + HALO + PAD
        return ref.at[:, pl.ds(begin * LANE, (end - begin) * LANE)]

    def to_partner_own(c):
        return remote(part(own, c), part(prev1, c), s_prev1.at[c], r_prev1.at[c], partner, n)

    def to_partner_forward(c):
        return remote(part(prev2, c), part(prev1, c), s_prev1.at[c], r_prev1.at[c], partner, n)

    def ahead_own(c):
        return remote(part(own, c), part(prev2, c), s_prev2.at[c], r_prev2.at[c], ahead, n)

    def ahead_forward(c):
        return remote(part(prev1, c), part(prev3, c), s_prev3.at[c], r_prev3.at[c], ahead, n)

    has_behind = p >= 2
    has_ahead = p + 2 < slices
    odd = jnp.logical_not(even)

    def start_ahead(c):
        @pl.when(has_ahead)
        def _():
            ahead_own(c).start()

    @pl.when(even)
    def _():
        for c in range(CHUNKS):
            to_partner_own(c).start()
    def pass_across(c):
        @pl.when(has_behind)
        def _():
            ahead_own(c).wait_recv()

        @pl.when(jnp.logical_and(odd, has_behind))
        def _():
            to_partner_forward(c).start()

    def pass_ahead(c):
        @pl.when(odd)
        def _():
            to_partner_own(c).wait_recv()

        @pl.when(jnp.logical_and(even, has_behind))
        def _():
            to_partner_forward(c).wait_recv()

        @pl.when(jnp.logical_and(has_ahead, jnp.logical_not(first)))
        def _():
            ahead_forward(c).start()

    for c in range(3):
        start_ahead(c)

    acc[...] = jnp.zeros_like(acc)

    def diffusion(v, c, k):
        size = (k + 2) * LANE
        right = pltpu.roll(v, size - 1, 1)
        flux = c * (right - v)
        left = pltpu.roll(flux, 1, 1)
        return (flux - left)[:, LANE:LANE + k * LANE]

    def two_steps(base, u, square, reaction, a):
        s = (3.0 * a) * square - a
        d = 1.0 + s
        top = base + u * s
        target = base - a * reaction
        dd = d * d
        tt = top * top
        above = target * (d * dd) + (2.0 * a) * (top * tt)
        below = d * ((1.0 - a) * dd + (3.0 * a) * tt)
        guess = pl.reciprocal(below, approx=True)
        return above * (guess * (2.0 - below * guess))

    def folded(value, k):
        out = value[:, :LANE]
        for piece in range(1, k):
            out = out + value[:, piece * LANE:(piece + 1) * LANE]
        return out

    def run(begin, end, block, counted):
        count = (end - begin) // STEP

        def step(i, carry):
            block(begin + i * STEP, STEP, counted)
            return carry

        lax.fori_loop(0, count, step, 0)
        if begin + count * STEP < end:
            block(begin + count * STEP, end - begin - count * STEP, counted)

    def over(c, lag, block):
        begin = c * tiles + lag if c else 0
        end = min((c + 1) * tiles + lag, all_tiles)
        if c == 0 and lag:
            block(-lag, lag, False)
        run(begin, end, block, True)
        if c == CHUNKS - 1 and lag:
            block(all_tiles, lag, False)

    def lanes(offset):
        return offset * LANE if isinstance(offset, int) else pl.multiple_of(offset * LANE, LANE)

    def wide(tile, k):
        return pl.ds(lanes(tile + PAD - 1), (k + 2) * LANE)

    def centre(tile, k):
        return pl.ds(lanes(tile + PAD), k * LANE)

    pass_across(0)
    pass_across(1)
    pass_ahead(0)
    for c in range(CHUNKS):
        base_lane = c * chunk

        if c + 3 < CHUNKS:
            start_ahead(c + 3)
        if c + 1 < CHUNKS:
            pass_ahead(c + 1)

        @pl.when(p >= 3)
        def _():
            ahead_forward(c).wait_recv()

        def stage_a(tile, k, counted):
            mid_slice = slice(LANE, LANE + k * LANE)
            cw = couple[:, wide(tile, k)]
            at = centre(tile, k)
            vw = own[:, wide(tile, k)]
            v = vw[:, mid_slice]
            p1w = jnp.where(first, vw, prev1[:, wide(tile, k)])
            p1 = p1w[:, mid_slice]
            p2w = jnp.where(p <= 1, p1w, prev2[:, wide(tile, k)])
            p2 = p2w[:, mid_slice]
            p3 = jnp.where(p <= 2, p2, prev3[:, at])

            square = v * v
            reaction = v - v * square
            forcing = diffusion(vw, cw, k) + reaction
            found = None
            for m in range(M):
                base = p1 + total[m] * forcing
                if counted:
                    defect = base - v
                    found = defect * defect if found is None else found + defect * defect
                here[m, :, at] = two_steps(base, v, square, reaction, implicit[m])
            if counted:
                acc[0] += folded(found, k)

            square = p1 * p1
            reaction = p1 - p1 * square
            forcing = diffusion(p1w, cw, k) + reaction
            for m in range(M):
                there[m, :, at] = two_steps(p2 + total[m] * forcing, p1, square, reaction, implicit[m])

            square = p2 * p2
            reaction = p2 - p2 * square
            forcing = diffusion(p2w, cw, k) + reaction
            last = two_steps(
                p3 + total[M - 1] * forcing, p2, square, reaction, implicit[M - 1]
            )
            before[:, at] = jnp.where(second, p1, last)

        over(c, 2, stage_a)
        if c + 2 < CHUNKS:
            pass_across(c + 2)

        def update(source, begin, cw, tile, k, which, counted):
            values = []
            forcings = []
            for m in range(M):
                vw = source[m, :, wide(tile, k)]
                v = vw[:, LANE:LANE + k * LANE]
                square = v * v
                reaction = v - v * square
                values.append((v, square, reaction))
                forcings.append(diffusion(vw, cw, k) + reaction)
            found = None
            outputs = []
            for m in range(M):
                base = begin
                for j in range(M):
                    base = base + weight[m][j] * forcings[j]
                v, square, reaction = values[m]
                if counted:
                    defect = base - v
                    found = defect * defect if found is None else found + defect * defect
                outputs.append(two_steps(base, v, square, reaction, implicit[m]))
            if counted:
                acc[which] += folded(found, k)
            return outputs

        def stage_b(tile, k, counted):
            cw = couple[:, wide(tile, k)]
            at = centre(tile, k)
            begin = jnp.where(first, own[:, centre(tile, k)], there[M - 1, :, at])
            outputs = update(here, begin, cw, tile, k, 1, counted)
            for m in range(M):
                mid[m, :, at] = outputs[m]
            mixed = None
            mixed_reaction = None
            for m in range(M):
                w = weight[M - 1][m]
                vw = there[m, :, wide(tile, k)]
                v = vw[:, LANE:LANE + k * LANE]
                square = v * v
                reaction = v - v * square
                mixed = w * vw if mixed is None else mixed + w * vw
                mixed_reaction = w * reaction if mixed_reaction is None else mixed_reaction + w * reaction
            base = before[:, at] + (diffusion(mixed, cw, k) + mixed_reaction)
            last = two_steps(base, v, square, reaction, implicit[M - 1])
            before[:, at] = jnp.where(first, own[:, centre(tile, k)], last)

        over(c, 1, stage_b)

        def stage_c(tile, k, counted):
            cw = couple[:, wide(tile, k)]
            outputs = update(mid, before[:, centre(tile, k)], cw, tile, k, 2, counted)
            at = pl.ds(lanes(tile - c * tiles), k * LANE)
            for m in range(M):
                result[c, m, :, at] = outputs[m]

        over(c, 0, stage_c)

        target = out_hbm.at[my_rows, pl.ds(base_lane, chunk)]
        for step in (2, 3, 1):
            peer = lax.rem(n + step, M)
            remote(result.at[c, peer], target, s_out.at[c, step], r_out.at[c, step], p, peer).start()
        pltpu.make_async_copy(result.at[c, n], target, local_sem.at[c]).start()

    lane = lax.broadcasted_iota(jnp.int32, (rows, LANE), 1)
    sub = lax.broadcasted_iota(jnp.int32, (rows, LANE), 0)
    place = lax.broadcasted_iota(jnp.int32, (8, LANE), 0)
    tile_value = jnp.zeros((8, LANE), jnp.float32)
    for which in range(3):
        per_system = jnp.sum(acc[which], axis=1, keepdims=True)
        row = jnp.sum(
            jnp.where(lane == n * rows + sub, per_system, 0.0), axis=0, keepdims=True
        )
        tile_value = tile_value + jnp.where(place == which, row, 0.0)
    part_tm[p] = tile_value
    sends = []
    for step in range(1, slices):
        copy = remote(
            part_tm.at[p], part_tm.at[p], s_tm.at[step], r_tm.at[step], lax.rem(p + step, slices), n
        )
        copy.start()
        sends.append(copy)
    for step in range(1, slices):
        source = lax.rem(p - step + slices, slices)
        remote(part_tm.at[source], part_tm.at[source], s_tm.at[step], r_tm.at[step], p, n).wait_recv()
    summed = part_tm[0]
    for index in range(1, slices):
        summed = summed + part_tm[index]
    part_node[n] = summed
    for step in range(1, M):
        copy = remote(
            part_node.at[n], part_node.at[n], s_node.at[step], r_node.at[step], p, lax.rem(n + step, M)
        )
        copy.start()
        sends.append(copy)
    for step in range(1, M):
        source = lax.rem(n - step + M, M)
        remote(part_node.at[source], part_node.at[source], s_node.at[step], r_node.at[step], p, n).wait_recv()
    summed = part_node[0]
    for index in range(1, M):
        summed = summed + part_node[index]
    log_ref[...] = jnp.log(log_floor + summed / (slices * M * cells))

    for copy in sends:
        copy.wait_send()
    for c in range(CHUNKS):
        here_rows = pl.ds(c * chunk, chunk)
        for step in range(1, M):
            source = lax.rem(n - step + M, M)
            landed = out_hbm.at[pl.ds(pl.multiple_of(source * rows, rows), rows), here_rows]
            arrived = remote(result.at[c, n], landed, s_out.at[c, step], r_out.at[c, step], p, n)
            arrived.wait_recv()
            arrived.wait_send()
        pltpu.make_async_copy(result.at[c, n], out_hbm.at[my_rows, here_rows], local_sem.at[c]).wait()

        @pl.when(has_ahead)
        def _():
            ahead_own(c).wait_send()

        @pl.when(jnp.logical_and(has_ahead, jnp.logical_not(first)))
        def _():
            ahead_forward(c).wait_send()

        @pl.when(even)
        def _():
            to_partner_own(c).wait_send()

        @pl.when(jnp.logical_and(odd, has_behind))
        def _():
            to_partner_forward(c).wait_send()


def solution(mesh):
    slices = mesh.shape["tm"]

    def body(slice_starts, coupling):
        systems, cells = coupling.shape
        rows = systems // M
        chunk = cells // CHUNKS
        padded = cells + 2 * PAD * LANE
        f32 = jnp.float32
        dma = pltpu.SemaphoreType.DMA
        anywhere = pl.BlockSpec(memory_space=pl.ANY)
        values, logs = pl.pallas_call(
            functools.partial(kernel, slices, rows, cells),
            out_shape=(
                jax.ShapeDtypeStruct((systems, cells), f32),
                jax.ShapeDtypeStruct((8, LANE), f32),
            ),
            in_specs=[anywhere, anywhere],
            out_specs=(anywhere, pl.BlockSpec(memory_space=pltpu.VMEM)),
            scratch_shapes=[
                pltpu.VMEM((rows, padded), f32),
                pltpu.VMEM((rows, padded), f32),
                pltpu.VMEM((rows, padded), f32),
                pltpu.VMEM((rows, padded), f32),
                pltpu.VMEM((rows, padded), f32),
                pltpu.VMEM((M, rows, padded), f32),
                pltpu.VMEM((M, rows, padded), f32),
                pltpu.VMEM((M, rows, padded), f32),
                pltpu.VMEM((rows, padded), f32),
                pltpu.VMEM((CHUNKS, M, rows, chunk), f32),
                pltpu.VMEM((3, rows, LANE), f32),
                pltpu.VMEM((slices, 8, LANE), f32),
                pltpu.VMEM((M, 8, LANE), f32),
                dma((2, 3)),
                dma((CHUNKS,)), dma((CHUNKS,)), dma((CHUNKS,)),
                dma((CHUNKS,)), dma((CHUNKS,)), dma((CHUNKS,)),
                dma((CHUNKS, M)), dma((CHUNKS, M)), dma((CHUNKS,)),
                dma((slices,)), dma((slices,)), dma((M,)), dma((M,)),
            ],
            compiler_params=pltpu.CompilerParams(
                collective_id=0, has_side_effects=True, vmem_limit_bytes=48 * 1024 * 1024
            ),
        )(slice_starts, coupling)
        return values[None, None], logs[:3, :systems]

    return jax.shard_map(
        body,
        mesh=mesh,
        in_specs=(P("tm", None, None), P()),
        out_specs=(P("tm", "node", None, None), P()),
        check_vma=False,
    )
```
